256 devices in a mesh: aux: 32 (over z, x), grp: 8 (over y, core).
Axes of the slice: x: 4, y: 4, z: 8, core: 2. Of those that a mesh axis runs over, the one named last changes fastest.
Arguments:
- source: float32 [1024, 256], P(('aux', 'grp')), may hold values from -6 to 6
- vir_energy: float32 [1024], P(('aux', 'grp')), may hold values from 0.5 to 3
- occ_energy: float32 [256], replicated, may hold values from -2 to -0.5
- factor_vv: float32 [512, 1024, 1024], P(('aux', 'grp')), may hold values from -0.75 to 0.75
- factor_oo: float32 [512, 256, 256], P(('aux', 'grp')), may hold values from -0.015625 to 0.015625
Outputs:
- response: float32 [1024, 256], P(('aux', 'grp'))
The draws below stay inside these ranges and needn't reach their ends.
All inputs are finite; a program needn't handle non-finite values.
Results may differ from the reference program's by a relative error of at most 0.0001.
Values sent between devices are 32-bit elements; how exact they have to be, the bound alone decides.
No kernel may reach another device: no remote copies, remote signals or barrier semaphores. Data moves between devices by JAX's collectives and lax.ppermute only.
A program may use at most 64 MiB of HBM per device.

```python
import jax
import jax.numpy as jnp
from jax import lax

NV = 1024
NO = 256
ITERS = 2
NAUX = 512


def with_spikes(entries, stream_key, source, target, parts, factor):
    owner, partner = [(jnp.arange(entries.shape[position]) // (entries.shape[position] // parts)).reshape([-1 if axis == position else 1 for axis in range(entries.ndim)]) for position in (source, target)]
    chosen = jax.random.permutation(stream_key, parts)[partner]
    strong = (owner == chosen) | (owner == (partner + parts // 2) % parts)
    return jnp.where(strong, factor * entries, entries)


def steps_of(own_key, extent, shards, smallest, largest):
    factor_of = 1.0
    for axis_at, parts in shards:
        draws = jax.random.uniform(jax.random.fold_in(jax.random.fold_in(own_key, 6), axis_at), (parts,), jnp.float32, smallest / len(shards), largest / len(shards))
        factor_of = factor_of * jnp.repeat(jnp.exp(draws), extent[axis_at] // parts).reshape((-1,) + (1,) * (len(extent) - 1 - axis_at))
    return factor_of


def centred(key, shape, spread, most, pieces=(), dtype=jnp.bfloat16):
    factor_of = steps_of(key, shape, pieces, -0.22, 0.18) if pieces else 1.0
    array = jax.random.normal(key, shape, jnp.float32) * spread * factor_of
    return jnp.minimum(jnp.maximum(array, -most), most).astype(dtype)


def noise_with(rng, extent, width, bound, split, heavy, dtype=jnp.bfloat16):
    array = width * jax.random.normal(rng, extent, jnp.float32)
    if split:
        array = array * steps_of(rng, extent, split, -0.22, 0.18)
    return jnp.clip(with_spikes(array, jax.random.fold_in(rng, 3), *heavy), -bound, bound).astype(dtype)


def setup_inputs(seed: int = 0) -> dict:
    seeds = jax.random.split(jax.random.key(seed), 6)
    source = centred(seeds[0], (NV, NO), 1.0, 6.0, ((0, 256),), jnp.float32)
    vir_energy = jnp.clip(0.5 + 2.5 * jax.random.uniform(seeds[1], (NV,), jnp.float32) ** steps_of(seeds[1], (NV,), ((0, 256),), -0.2, 0.2), 0.5, 3.0)
    occ_energy = jnp.clip(jax.random.uniform(seeds[2], (NO,), jnp.float32, -2.0, -0.5), -2.0, -0.5)
    factor_vv = noise_with(seeds[3], (NAUX, NV, NV), NV ** -0.5, 0.75, ((0, 256),), (0, 1, 256, 6.0), jnp.float32)
    factor_oo = centred(seeds[4], (NAUX, NO, NO), (NO * NAUX) ** -0.5, 0.015625, ((0, 256),), jnp.float32)
    return {"source": source, "vir_energy": vir_energy, "occ_energy": occ_energy, "factor_vv": factor_vv, "factor_oo": factor_oo}


def apply_factors(amplitudes, factor_vv, factor_oo):
    def step(total, pair):
        left, right = pair
        inner = jnp.dot(left, amplitudes, precision=lax.Precision.HIGHEST, preferred_element_type=jnp.float32)
        return total + jnp.dot(inner, right, precision=lax.Precision.HIGHEST, preferred_element_type=jnp.float32), None

    start = jnp.zeros(amplitudes.shape, jnp.float32)
    total, _ = lax.scan(step, start, (factor_vv, factor_oo))
    return total


def reference(source, vir_energy, occ_energy, factor_vv, factor_oo):
    gap = vir_energy[:, None] - occ_energy[None, :]
    amplitudes = source / gap
    for sweep in range(ITERS):
        summed = apply_factors(amplitudes, factor_vv, factor_oo)
        amplitudes = (source - summed) / gap
    return amplitudes
```

```python
import itertools

import jax
import jax.numpy as jnp
from jax import lax
from jax.experimental import pallas as pl
from jax.experimental.pallas import tpu as pltpu
from jax.sharding import Mesh
from jax.sharding import PartitionSpec as P

ITERS = 2
SHAPE = (8, 4, 4, 2)
BLOCKS = 4
MIB = 1024 * 1024
VMEM = pl.BlockSpec(memory_space=pltpu.VMEM)
SMEM = pl.BlockSpec(memory_space=pltpu.SMEM)


def shaped(shape, dtype=jnp.float32):
    return jax.ShapeDtypeStruct(shape, dtype)


def call(kernel, out_shape, in_specs, mib, scratch=(), cost=None):
    return pl.pallas_call(
        kernel,
        out_shape=out_shape,
        in_specs=in_specs,
        out_specs=jax.tree.map(lambda _: VMEM, out_shape),
        scratch_shapes=scratch,
        cost_estimate=cost,
        compiler_params=pltpu.CompilerParams(vmem_limit_bytes=mib * MIB),
    )


def split(value):
    high = value.astype(jnp.bfloat16)
    low = (value - high.astype(jnp.float32)).astype(jnp.bfloat16)
    return high, low


def product(left, right):
    return jnp.dot(left, right, preferred_element_type=jnp.float32)


def split_kernel(value, high, low):
    high[...], low[...] = split(value[...])


def split_blocks(value):
    pairs, rows, cols = value.shape
    block = pl.BlockSpec((1, rows // BLOCKS, cols), lambda p, n: (p, n, 0))
    out = shaped(value.shape, jnp.bfloat16)
    return pl.pallas_call(
        split_kernel,
        grid=(pairs, BLOCKS),
        in_specs=[block],
        out_specs=(block, block),
        out_shape=(out, out),
        compiler_params=pltpu.CompilerParams(vmem_limit_bytes=12 * MIB),
    )(value)


def core_of(spot):
    return lax.rem(spot[0], 2)


def packed_kernel(spot, vir, source, occ, send, mine):
    rows, cols = source.shape
    half = cols // 2
    first = core_of(spot) == 0
    row = lax.broadcasted_iota(jnp.int32, (rows, cols), 0)
    levels = jnp.full((rows, cols), vir[0])
    for r in range(1, rows):
        levels = jnp.where(row == r, vir[r], levels)
    for at, value in ((0, source[...]), (rows, levels - occ[...])):
        left, right = value[:, :half], value[:, half:]
        send[at : at + rows, :] = jnp.where(first, right, left)
        mine[at : at + rows, :] = jnp.where(first, left, right)


def start_kernel(spot, mine, arrived, block, gap, copies):
    rows = mine.shape[0] // 2
    first = core_of(spot) == 0
    ours, theirs = mine[...], arrived[...]

    def ordered(part):
        here, there = ours[part, :], theirs[part, :]
        return jnp.where(
            first, jnp.concatenate([here, there]), jnp.concatenate([there, here])
        )

    value, spread = ordered(slice(0, rows)), ordered(slice(rows, 2 * rows))
    block[...] = value
    gap[...] = spread
    for n in range(copies.shape[0]):
        copies[n, 0] = value
        copies[n, 1] = spread


def first_kernel(given, copies):
    value = given[:, 0] / given[:, 1]
    for n in range(copies.shape[0]):
        copies[n] = value


def summed(arrived):
    total = arrived[0]
    for n in range(1, arrived.shape[0]):
        total = total + arrived[n]
    return total


def spread_kernel(arrived, copies):
    total = summed(arrived)
    for n in range(copies.shape[0]):
        copies[n] = total


def next_kernel(given, arrived, copies):
    value = (given[:, 0] - summed(arrived)) / given[:, 1]
    for n in range(copies.shape[0]):
        copies[n] = value


def total_kernel(arrived, out):
    out[...] = summed(arrived)


def last_kernel(spot, block, gap, arrived, mine, send):
    rows = mine.shape[0]
    first = core_of(spot) == 0
    value = (block[...] - summed(arrived)) / gap[...]
    top, bottom = value[:rows, :], value[rows:, :]
    mine[...] = jnp.where(first, top, bottom)
    send[...] = jnp.where(first, bottom, top)


def turned_kernel(spot, factor, high, low):
    half = factor.shape[1] // 2
    first = core_of(spot) == 0
    value = factor[...]
    value = jnp.where(
        first, value, jnp.concatenate([value[:, half:, :], value[:, :half, :]], axis=1)
    )
    value = jnp.where(
        first, value, jnp.concatenate([value[..., half:], value[..., :half]], axis=2)
    )
    high[...], low[...] = split(value)


def terms_kernel(own, other, oo_high, oo_low, vv_high, vv_low, keep, send, half_high, half_low):
    pairs, rows, _ = vv_high.shape
    near, planes, tile, width = keep.shape
    chunk = near * tile
    group = 2

    def natural(ref, n):
        return jnp.concatenate(
            [ref[:, z, :, :].reshape(chunk, width) for z in range(n * group, (n + 1) * group)]
        )

    for n in range(planes // group):
        part = pl.ds(n * group * chunk, group * chunk)
        high, low = split(jnp.concatenate([natural(own, n), natural(other, n)], axis=1))
        for p in range(pairs):
            halfway = (
                product(high, oo_low[p]) + product(low, oo_high[p]) + product(high, oo_high[p])
            )
            half_high[p, part, :], half_low[p, part, :] = split(halfway)
    for n in range(planes // group):
        part = pl.ds(n * group * chunk, group * chunk)
        total = None
        for p in range(pairs):
            high, low = vv_high[p, part, :], vv_low[p, part, :]
            term = (
                product(high, half_low[p]) + product(low, half_high[p]) + product(high, half_high[p])
            )
            total = term if total is None else total + term
        for m in range(group):
            piece = total[m * chunk : (m + 1) * chunk, :]
            keep[:, n * group + m, :, :] = piece[:, :width].reshape(near, tile, width)
            send[:, n * group + m, :, :] = piece[:, width:].reshape(near, tile, width)


def partial_terms(own, other, oo, vv):
    pairs, rows, _ = vv[0].shape
    out = shaped(own.shape)
    halfway = pltpu.VMEM((pairs, rows, 2 * own.shape[-1]), jnp.bfloat16)
    kernel = call(terms_kernel, (out, out), [VMEM] * 6, 24, (halfway, halfway))
    return kernel(own, other, *oo, *vv)


def device(z, x, y, c):
    _, xs, ys, cores = SHAPE
    return ((z * xs + x) * ys + y) * cores + c


def every():
    return itertools.product(*(range(n) for n in SHAPE))


def swapped(value):
    pairs = [(device(z, x, y, c), device(z, x, y, 1 - c)) for z, x, y, c in every()]
    return lax.ppermute(value, "d", pairs)


def exchanged(value, kept):
    groups = {}
    for spot in every():
        groups.setdefault(tuple(spot[k] for k in kept), []).append(device(*spot))
    groups = list(groups.values())
    return lax.all_to_all(value, "d", 0, 0, axis_index_groups=groups, tiled=True)


def along_z(value):
    return exchanged(value, (1, 2, 3))


def along_xy(value):
    return exchanged(value, (0, 3))


def local(source, vir_energy, occ_energy, factor_vv, factor_oo):
    spot = lax.axis_index("d").astype(jnp.int32).reshape(1)
    first = lax.rem(spot[0], 2) == 0
    planes, xs, ys, _ = SHAPE
    near = xs * ys
    rows, cols = source.shape
    half = cols // 2

    tile = (2 * rows, half)
    one = shaped(tile)
    send, mine = call(packed_kernel, (one, one), [SMEM, SMEM, VMEM, VMEM], 60)(
        spot, vir_energy, source, occ_energy[None]
    )
    block, gap, copies = call(
        start_kernel, (one, one, shaped((planes, 2, *tile))), [SMEM] + [VMEM] * 2, 4
    )(spot, mine, swapped(send))

    oo = shaped(factor_oo.shape, jnp.bfloat16)
    oo = call(turned_kernel, (oo, oo), [SMEM, VMEM], 8)(spot, factor_oo)
    vv = split_blocks(factor_vv)

    given = along_z(copies)
    plane_copies = shaped((planes, planes, *tile))
    near_copies = shaped((near, planes, *tile))
    long = pl.CostEstimate(flops=10**10, bytes_accessed=10**7, transcendentals=0)
    copies = call(first_kernel, near_copies, [VMEM], 4, cost=long)(given)
    for sweep in range(ITERS):
        if sweep:
            arrived = along_z(call(spread_kernel, plane_copies, [VMEM], 4)(arrived))
            copies = call(next_kernel, near_copies, [VMEM] * 2, 4)(given, arrived)
        own = along_xy(copies)
        keep, send = partial_terms(own, swapped(own), oo, vv)
        arrived = along_xy(keep + swapped(send))
    arrived = along_z(call(total_kernel, shaped((planes, *tile)), [VMEM], 4)(arrived))
    part = shaped((rows, half))
    mine, send = call(last_kernel, (part, part), [SMEM] + [VMEM] * 3, 4)(spot, block, gap, arrived)
    partner = swapped(send)
    return jnp.where(
        first,
        jnp.concatenate([mine, partner], axis=1),
        jnp.concatenate([partner, mine], axis=1),
    )


def solution(mesh):
    line = Mesh(mesh.devices.reshape(-1), ("d",))
    placed = (P("d", None), P("d"), P(), P("d", None, None), P("d", None, None))
    return jax.shard_map(
        local, mesh=line, in_specs=placed, out_specs=P("d", None), check_vma=False
    )
```

```python
import itertools

import jax
import jax.numpy as jnp
from jax import lax
from jax.experimental import pallas as pl
from jax.experimental.pallas import tpu as pltpu
from jax.sharding import Mesh
from jax.sharding import PartitionSpec as P

ITERS = 2
SHAPE = (8, 4, 4, 2)
PLANES, NEAR, CORES = 8, 16, 2
MIB = 1024 * 1024
VMEM = pl.BlockSpec(memory_space=pltpu.VMEM)


def shaped(shape, dtype=jnp.float32):
    return jax.ShapeDtypeStruct(shape, dtype)


def call(kernel, out_shape, in_specs, mib, flops=0):
    cost = pl.CostEstimate(flops=flops, bytes_accessed=10**7, transcendentals=0)
    return pl.pallas_call(
        kernel,
        out_shape=out_shape,
        in_specs=in_specs,
        out_specs=jax.tree.map(lambda _: VMEM, out_shape),
        cost_estimate=cost if flops else None,
        compiler_params=pltpu.CompilerParams(vmem_limit_bytes=mib * MIB),
    )


def split(value):
    high = value.astype(jnp.bfloat16)
    low = (value - high.astype(jnp.float32)).astype(jnp.bfloat16)
    return high, low


def product(left, right):
    return jnp.dot(left, right, preferred_element_type=jnp.float32)


def interleaved(top, bottom):
    axis = top.ndim - 2
    head = lax.broadcasted_iota(jnp.int32, top.shape, axis) < 4
    return (
        jnp.where(head, top, pltpu.roll(bottom, 4, axis)),
        jnp.where(head, pltpu.roll(top, 4, axis), bottom),
    )


def split_kernel(value, high, low):
    def tile_at(z, at):
        return value[0, pl.ds(pl.multiple_of((z * NEAR + at) * 8, 8), 8), :]

    def step(at, carry):
        cores = ([], [])
        for z in range(0, value.shape[1] // (NEAR * 8), 2):
            for core, tile in enumerate(interleaved(tile_at(z, at), tile_at(z + 1, at))):
                cores[core].append(tile)
        for core, tiles in enumerate(cores):
            high[0, core, at], low[0, core, at] = split(jnp.concatenate(tiles))
        return carry

    lax.fori_loop(0, NEAR, step, 0, unroll=4)


def split_blocks(value):
    pairs, rows, cols = value.shape
    out = shaped((pairs, CORES, NEAR, PLANES * 4, cols), jnp.bfloat16)
    block = pl.BlockSpec((1, CORES, NEAR, 16, cols), lambda p, n: (p, 0, 0, n, 0))
    return pl.pallas_call(
        split_kernel,
        grid=(pairs, PLANES // 4),
        in_specs=[pl.BlockSpec((1, 4 * NEAR * 8, cols), lambda p, n: (p, n, 0))],
        out_specs=(block, block),
        out_shape=(out, out),
        compiler_params=pltpu.CompilerParams(vmem_limit_bytes=12 * MIB),
    )(value)


def summed(arrived):
    total = arrived[0]
    for n in range(1, arrived.shape[0]):
        total = total + arrived[n]
    return total


def spread(value, copies):
    for n in range(copies.shape[0]):
        copies[n] = value


def first_kernel(given, source, gap, copies):
    for z in range(0, PLANES, 2):
        part = slice(4 * z, 4 * z + 8)
        source[part, :] = jnp.concatenate([given[z, 0], given[z + 1, 0]])
        gap[part, :] = jnp.concatenate([given[z, 1], given[z + 1, 1]])
    spread(source[...] / gap[...], copies)


def partial_kernel(arrived, copies):
    spread(summed(arrived), copies)


def next_kernel(source, gap, arrived, copies):
    spread((source[...] - summed(arrived)) / gap[...], copies)


def total_kernel(arrived, out):
    total = summed(arrived)
    for z in range(PLANES):
        out[z] = total[4 * z : 4 * z + 4, :]


def last_kernel(both, arrived, out):
    out[...] = (both[0] - summed(arrived)) / both[1]


def left_products(core, vv_high, vv_low, half_high, half_low, out):
    group = 8
    for n in range(0, NEAR, group):
        total = None
        for p in range(vv_high.shape[0]):
            high, low = (
                vv[p, core, n : n + group].reshape(group * PLANES * 4, -1)
                for vv in (vv_high, vv_low)
            )
            term = (
                product(high, half_low[p]) + product(low, half_high[p]) + product(high, half_high[p])
            )
            total = term if total is None else total + term
        out[n : n + group] = total.reshape(group, PLANES * 4, -1)


def send_kernel(own, other, oo, vv_high, vv_low, send, half_high, half_low):
    core = lax.rem(lax.axis_index("d"), CORES)
    first = core == 0
    for z in range(0, PLANES, 2):
        part = slice(4 * z, 4 * z + 8)
        ours, theirs = own[:, part, :], other[:, part, :]
        planes = interleaved(jnp.where(first, ours, theirs), jnp.where(first, theirs, ours))
        high, low = split(jnp.concatenate([v.reshape(NEAR * 8, -1) for v in planes]))
        rows = slice(z * NEAR * 8, (z + 2) * NEAR * 8)
        for p in range(oo.shape[0]):
            oo_high, oo_low = split(oo[p])
            halfway = product(high, oo_low) + product(low, oo_high) + product(high, oo_high)
            half_high[p, rows, :], half_low[p, rows, :] = split(halfway)
    left_products(1 - core, vv_high, vv_low, half_high, half_low, send)


def keep_kernel(vv_high, vv_low, half_high, half_low, keep):
    core = lax.rem(lax.axis_index("d"), CORES)
    left_products(core, vv_high, vv_low, half_high, half_low, keep)


def device(z, x, y, c):
    _, xs, ys, cores = SHAPE
    return ((z * xs + x) * ys + y) * cores + c


def every():
    return itertools.product(*(range(n) for n in SHAPE))


def swapped(value):
    pairs = [(device(z, x, y, c), device(z, x, y, 1 - c)) for z, x, y, c in every()]
    return lax.ppermute(value, "d", pairs)


def exchanged(value, kept):
    groups = {}
    for spot in every():
        groups.setdefault(tuple(spot[k] for k in kept), []).append(device(*spot))
    groups = list(groups.values())
    return lax.all_to_all(value, "d", 0, 0, axis_index_groups=groups, tiled=True)


def along_z(value):
    return exchanged(value, (1, 2, 3))


def along_xy(value):
    return exchanged(value, (0, 3))


def local(source, vir_energy, occ_energy, factor_vv, factor_oo):
    rows, cols = source.shape
    pairs = factor_oo.shape[0]

    shape = (2, rows, cols)
    gap = lax.broadcast_in_dim(vir_energy, shape, (1,)) - lax.broadcast_in_dim(occ_energy, shape, (2,))
    which = lax.broadcasted_iota(jnp.int32, shape, 0)
    both = jnp.where(which == 0, lax.broadcast_in_dim(source, shape, (1, 2)), gap)
    both = lax.optimization_barrier(both)
    vv = split_blocks(factor_vv)

    plane = shaped((PLANES * rows, cols))
    near = shaped((NEAR, *plane.shape))
    planes = shaped((PLANES, *plane.shape))
    half = shaped((pairs, NEAR * PLANES * 8, cols), jnp.bfloat16)
    given = along_z(jnp.broadcast_to(both[None], (PLANES, *both.shape)))
    all_source, all_gap, copies = call(first_kernel, (plane, plane, near), [VMEM], 4, 10**10)(given)
    for sweep in range(ITERS):
        if sweep:
            arrived = along_z(call(partial_kernel, planes, [VMEM], 4)(arrived))
            copies = call(next_kernel, near, [VMEM] * 3, 4)(all_source, all_gap, arrived)
        own = along_xy(copies)
        send, *halves = call(send_kernel, (near, half, half), [VMEM] * 5, 24, 10**9)(
            own, swapped(own), factor_oo, *vv
        )
        arrived = swapped(send)
        keep = call(keep_kernel, near, [VMEM] * 4, 24, 10**9)(*vv, *halves)
        arrived = along_xy(keep + arrived)
    arrived = along_z(call(total_kernel, shaped((PLANES, rows, cols)), [VMEM], 4)(arrived))
    return call(last_kernel, shaped((rows, cols)), [VMEM] * 2, 4)(both, arrived)


def solution(mesh):
    line = Mesh(mesh.devices.reshape(-1), ("d",))
    placed = (P("d", None), P("d"), P(), P("d", None, None), P("d", None, None))
    return jax.shard_map(
        local, mesh=line, in_specs=placed, out_specs=P("d", None), check_vma=False
    )
```

```python
import itertools

import jax
import jax.numpy as jnp
from jax import lax
from jax.experimental import pallas as pl
from jax.experimental.pallas import tpu as pltpu
from jax.sharding import Mesh
from jax.sharding import PartitionSpec as P

ITERS = 2
SHAPE = (8, 4, 4, 2)
PLANES, NEAR, CORES = 8, 16, 2
CHIPS = ((0, 0), (1, 0), (1, 1), (1, 2), (2, 2), (2, 1), (2, 0), (3, 0))
CHIPS += ((3, 1), (3, 2), (3, 3), (2, 3), (1, 3), (0, 3), (0, 2), (0, 1))
XY = tuple(x * SHAPE[2] + y for x, y in CHIPS)
Z = (0, 4, 2, 6, 1, 5, 3, 7)
MIB = 1024 * 1024
VMEM = pl.BlockSpec(memory_space=pltpu.VMEM)


def shaped(shape, dtype=jnp.float32):
    return jax.ShapeDtypeStruct(shape, dtype)


def call(kernel, out_shape, in_specs, mib, flops=0):
    cost = pl.CostEstimate(flops=flops, bytes_accessed=10**7, transcendentals=0)
    return pl.pallas_call(
        kernel,
        out_shape=out_shape,
        in_specs=in_specs,
        out_specs=jax.tree.map(lambda _: VMEM, out_shape),
        cost_estimate=cost if flops else None,
        compiler_params=pltpu.CompilerParams(vmem_limit_bytes=mib * MIB),
    )


def split(value):
    high = value.astype(jnp.bfloat16)
    low = (value - high.astype(jnp.float32)).astype(jnp.bfloat16)
    return high, low


def product(left, right):
    return jnp.dot(left, right, preferred_element_type=jnp.float32)


def interleaved(top, bottom):
    axis = top.ndim - 2
    head = lax.broadcasted_iota(jnp.int32, top.shape, axis) < 4
    return (
        jnp.where(head, top, pltpu.roll(bottom, 4, axis)),
        jnp.where(head, pltpu.roll(top, 4, axis), bottom),
    )


def split_kernel(value, high, low):
    def tile_at(z, at):
        return value[0, pl.ds((z * NEAR + at) * 8, 8), :]

    for n, at in enumerate(XY):
        cores = ([], [])
        for z in range(0, value.shape[1] // (NEAR * 8), 2):
            for core, tile in enumerate(interleaved(tile_at(z, at), tile_at(z + 1, at))):
                cores[core].append(tile)
        for core, tiles in enumerate(cores):
            high[0, core, n], low[0, core, n] = split(jnp.concatenate(tiles))


def split_blocks(value):
    pairs, rows, cols = value.shape
    out = shaped((pairs, CORES, NEAR, PLANES * 4, cols), jnp.bfloat16)
    block = pl.BlockSpec((1, CORES, NEAR, 16, cols), lambda p, n: (p, 0, 0, n, 0))
    return pl.pallas_call(
        split_kernel,
        grid=(pairs, PLANES // 4),
        in_specs=[pl.BlockSpec((1, 4 * NEAR * 8, cols), lambda p, n: (p, n, 0))],
        out_specs=(block, block),
        out_shape=(out, out),
        compiler_params=pltpu.CompilerParams(vmem_limit_bytes=12 * MIB),
    )(value)


def summed(arrived):
    total = arrived[0]
    for n in range(1, arrived.shape[0]):
        total = total + arrived[n]
    return total


def spread(value, copies):
    for n in range(copies.shape[0]):
        copies[n] = value


def first_kernel(given, source, gap, copies):
    for z in range(0, PLANES, 2):
        part = slice(4 * z, 4 * z + 8)
        at = Z.index(z), Z.index(z + 1)
        source[part, :] = jnp.concatenate([given[n, 0] for n in at])
        gap[part, :] = jnp.concatenate([given[n, 1] for n in at])
    spread(source[...] / gap[...], copies)


def partial_kernel(arrived, copies):
    spread(summed(arrived), copies)


def next_kernel(source, gap, arrived, copies):
    spread((source[...] - summed(arrived)) / gap[...], copies)


def total_kernel(arrived, out):
    total = summed(arrived)
    for n, z in enumerate(Z):
        out[n] = total[4 * z : 4 * z + 4, :]


def last_kernel(both, arrived, out):
    out[...] = (both[0] - summed(arrived)) / both[1]


def left_products(core, vv_high, vv_low, half_high, half_low, out):
    group = 8
    for n in range(0, NEAR, group):
        total = None
        for p in range(vv_high.shape[0]):
            high, low = (
                vv[p, core, n : n + group].reshape(group * PLANES * 4, -1)
                for vv in (vv_high, vv_low)
            )
            term = (
                product(high, half_low[p]) + product(low, half_high[p]) + product(high, half_high[p])
            )
            total = term if total is None else total + term
        out[n : n + group] = total.reshape(group, PLANES * 4, -1)


def send_kernel(own, other, oo, vv_high, vv_low, send, half_high, half_low):
    core = lax.rem(lax.axis_index("d"), CORES)
    first = core == 0
    for z in range(0, PLANES, 2):
        part = slice(4 * z, 4 * z + 8)
        ours, theirs = own[:, part, :], other[:, part, :]
        planes = interleaved(jnp.where(first, ours, theirs), jnp.where(first, theirs, ours))
        tiles = [v[XY.index(at)] for v in planes for at in range(NEAR)]
        high, low = split(jnp.concatenate(tiles))
        rows = slice(z * NEAR * 8, (z + 2) * NEAR * 8)
        for p in range(oo.shape[0]):
            oo_high, oo_low = split(oo[p])
            halfway = product(high, oo_low) + product(low, oo_high) + product(high, oo_high)
            half_high[p, rows, :], half_low[p, rows, :] = split(halfway)
    left_products(1 - core, vv_high, vv_low, half_high, half_low, send)


def keep_kernel(vv_high, vv_low, half_high, half_low, keep):
    core = lax.rem(lax.axis_index("d"), CORES)
    left_products(core, vv_high, vv_low, half_high, half_low, keep)


def device(z, x, y, c):
    _, xs, ys, cores = SHAPE
    return ((z * xs + x) * ys + y) * cores + c


def every():
    return itertools.product(*(range(n) for n in SHAPE))


def swapped(value):
    pairs = [(device(z, x, y, c), device(z, x, y, 1 - c)) for z, x, y, c in every()]
    return lax.ppermute(value, "d", pairs)


def exchanged(value, kept):
    groups = {}
    for spot in sorted(every(), key=lambda s: (Z.index(s[0]), CHIPS.index(s[1:3]), s[3])):
        groups.setdefault(tuple(spot[k] for k in kept), []).append(device(*spot))
    groups = list(groups.values())
    return lax.all_to_all(value, "d", 0, 0, axis_index_groups=groups, tiled=True)


def along_z(value):
    return exchanged(value, (1, 2, 3))


def along_xy(value):
    return exchanged(value, (0, 3))


def local(source, vir_energy, occ_energy, factor_vv, factor_oo):
    rows, cols = source.shape
    pairs = factor_oo.shape[0]

    shape = (2, rows, cols)
    gap = lax.broadcast_in_dim(vir_energy, shape, (1,)) - lax.broadcast_in_dim(occ_energy, shape, (2,))
    which = lax.broadcasted_iota(jnp.int32, shape, 0)
    both = jnp.where(which == 0, lax.broadcast_in_dim(source, shape, (1, 2)), gap)
    both = lax.optimization_barrier(both)
    vv = split_blocks(factor_vv)

    plane = shaped((PLANES * rows, cols))
    near = shaped((NEAR, *plane.shape))
    planes = shaped((PLANES, *plane.shape))
    half = shaped((pairs, NEAR * PLANES * 8, cols), jnp.bfloat16)
    given = along_z(jnp.broadcast_to(both[None], (PLANES, *both.shape)))
    all_source, all_gap, copies = call(first_kernel, (plane, plane, near), [VMEM], 4, 10**10)(given)
    for sweep in range(ITERS):
        if sweep:
            arrived = along_z(call(partial_kernel, planes, [VMEM], 4)(arrived))
            copies = call(next_kernel, near, [VMEM] * 3, 4)(all_source, all_gap, arrived)
        own = along_xy(copies)
        send, *halves = call(send_kernel, (near, half, half), [VMEM] * 5, 24, 10**9)(
            own, swapped(own), factor_oo, *vv
        )
        arrived = swapped(send)
        keep = call(keep_kernel, near, [VMEM] * 4, 24, 10**9)(*vv, *halves)
        arrived = along_xy(keep + arrived)
    arrived = along_z(call(total_kernel, shaped((PLANES, rows, cols)), [VMEM], 4)(arrived))
    return call(last_kernel, shaped((rows, cols)), [VMEM] * 2, 4)(both, arrived)


def solution(mesh):
    line = Mesh(mesh.devices.reshape(-1), ("d",))
    placed = (P("d", None), P("d"), P(), P("d", None, None), P("d", None, None))
    return jax.shard_map(
        local, mesh=line, in_specs=placed, out_specs=P("d", None), check_vma=False
    )
```

```python
import itertools

import jax
import jax.numpy as jnp
from jax import lax
from jax.experimental import pallas as pl
from jax.experimental.pallas import tpu as pltpu
from jax.sharding import Mesh
from jax.sharding import PartitionSpec as P

ITERS = 2
SHAPE = (8, 4, 4, 2)
PLANES, NEAR, CORES = 8, 16, 2
CHIPS = ((0, 0), (0, 1), (1, 1), (2, 1), (2, 2), (1, 2), (0, 2), (0, 3))
CHIPS += ((1, 3), (2, 3), (3, 3), (3, 2), (3, 1), (3, 0), (2, 0), (1, 0))
XY = tuple(x * SHAPE[2] + y for x, y in CHIPS)
Z = (0, 4, 2, 6, 1, 5, 3, 7)
MIB = 1024 * 1024
VMEM = pl.BlockSpec(memory_space=pltpu.VMEM)


def shaped(shape, dtype=jnp.float32):
    return jax.ShapeDtypeStruct(shape, dtype)


def call(kernel, out_shape, in_specs, mib, flops=0):
    cost = pl.CostEstimate(flops=flops, bytes_accessed=10**7, transcendentals=0)
    return pl.pallas_call(
        kernel,
        out_shape=out_shape,
        in_specs=in_specs,
        out_specs=jax.tree.map(lambda _: VMEM, out_shape),
        cost_estimate=cost if flops else None,
        compiler_params=pltpu.CompilerParams(vmem_limit_bytes=mib * MIB),
    )


def split(value):
    high = value.astype(jnp.bfloat16)
    low = (value - high.astype(jnp.float32)).astype(jnp.bfloat16)
    return high, low


def product(left, right):
    return jnp.dot(left, right, preferred_element_type=jnp.float32)


def interleaved(top, bottom):
    axis = top.ndim - 2
    head = lax.broadcasted_iota(jnp.int32, top.shape, axis) < 4
    return (
        jnp.where(head, top, pltpu.roll(bottom, 4, axis)),
        jnp.where(head, pltpu.roll(top, 4, axis), bottom),
    )


def split_kernel(value, high, low):
    def tile_at(z, at):
        return value[0, pl.ds((z * NEAR + at) * 8, 8), :]

    for n, at in enumerate(XY):
        cores = ([], [])
        for z in range(0, value.shape[1] // (NEAR * 8), 2):
            for core, tile in enumerate(interleaved(tile_at(z, at), tile_at(z + 1, at))):
                cores[core].append(tile)
        for core, tiles in enumerate(cores):
            high[0, core, n], low[0, core, n] = split(jnp.concatenate(tiles))


def split_blocks(value):
    pairs, rows, cols = value.shape
    out = shaped((pairs, CORES, NEAR, PLANES * 4, cols), jnp.bfloat16)
    block = pl.BlockSpec((1, CORES, NEAR, 16, cols), lambda p, n: (p, 0, 0, n, 0))
    return pl.pallas_call(
        split_kernel,
        grid=(pairs, PLANES // 4),
        in_specs=[pl.BlockSpec((1, 4 * NEAR * 8, cols), lambda p, n: (p, n, 0))],
        out_specs=(block, block),
        out_shape=(out, out),
        compiler_params=pltpu.CompilerParams(vmem_limit_bytes=12 * MIB),
    )(value)


def summed(arrived):
    total = arrived[0]
    for n in range(1, arrived.shape[0]):
        total = total + arrived[n]
    return total


def spread(value, copies):
    for n in range(copies.shape[0]):
        copies[n] = value


def first_kernel(given, source, gap, copies):
    for z in range(0, PLANES, 2):
        part = slice(4 * z, 4 * z + 8)
        at = Z.index(z), Z.index(z + 1)
        source[part, :] = jnp.concatenate([given[n, 0] for n in at])
        gap[part, :] = jnp.concatenate([given[n, 1] for n in at])
    spread(source[...] / gap[...], copies)


def partial_kernel(arrived, copies):
    spread(summed(arrived), copies)


def next_kernel(source, gap, arrived, copies):
    spread((source[...] - summed(arrived)) / gap[...], copies)


def total_kernel(arrived, out):
    total = summed(arrived)
    for n, z in enumerate(Z):
        out[n] = total[4 * z : 4 * z + 4, :]


def last_kernel(both, arrived, out):
    out[...] = (both[0] - summed(arrived)) / both[1]


def left_products(core, vv_high, vv_low, half_high, half_low, out):
    group = 8
    for n in range(0, NEAR, group):
        total = None
        for p in range(vv_high.shape[0]):
            high, low = (
                vv[p, core, n : n + group].reshape(group * PLANES * 4, -1)
                for vv in (vv_high, vv_low)
            )
            term = (
                product(high, half_low[p]) + product(low, half_high[p]) + product(high, half_high[p])
            )
            total = term if total is None else total + term
        out[n : n + group] = total.reshape(group, PLANES * 4, -1)


def send_kernel(own, other, oo, vv_high, vv_low, send, half_high, half_low):
    core = lax.rem(lax.axis_index("d"), CORES)
    first = core == 0
    for z in range(0, PLANES, 2):
        part = slice(4 * z, 4 * z + 8)
        ours, theirs = own[:, part, :], other[:, part, :]
        planes = interleaved(jnp.where(first, ours, theirs), jnp.where(first, theirs, ours))
        tiles = [v[XY.index(at)] for v in planes for at in range(NEAR)]
        high, low = split(jnp.concatenate(tiles))
        rows = slice(z * NEAR * 8, (z + 2) * NEAR * 8)
        for p in range(oo.shape[0]):
            oo_high, oo_low = split(oo[p])
            halfway = product(high, oo_low) + product(low, oo_high) + product(high, oo_high)
            half_high[p, rows, :], half_low[p, rows, :] = split(halfway)
    left_products(1 - core, vv_high, vv_low, half_high, half_low, send)


def keep_kernel(vv_high, vv_low, half_high, half_low, keep):
    core = lax.rem(lax.axis_index("d"), CORES)
    left_products(core, vv_high, vv_low, half_high, half_low, keep)


def device(z, x, y, c):
    _, xs, ys, cores = SHAPE
    return ((z * xs + x) * ys + y) * cores + c


def every():
    return itertools.product(*(range(n) for n in SHAPE))


def swapped(value):
    pairs = [(device(z, x, y, c), device(z, x, y, 1 - c)) for z, x, y, c in every()]
    return lax.ppermute(value, "d", pairs)


def exchanged(value, kept):
    groups = {}
    for spot in sorted(every(), key=lambda s: (Z.index(s[0]), CHIPS.index(s[1:3]), s[3])):
        groups.setdefault(tuple(spot[k] for k in kept), []).append(device(*spot))
    groups = list(groups.values())
    return lax.all_to_all(value, "d", 0, 0, axis_index_groups=groups, tiled=True)


def along_z(value):
    return exchanged(value, (1, 2, 3))


def along_xy(value):
    return exchanged(value, (0, 3))


def local(source, vir_energy, occ_energy, factor_vv, factor_oo):
    rows, cols = source.shape
    pairs = factor_oo.shape[0]

    shape = (2, rows, cols)
    gap = lax.broadcast_in_dim(vir_energy, shape, (1,)) - lax.broadcast_in_dim(occ_energy, shape, (2,))
    which = lax.broadcasted_iota(jnp.int32, shape, 0)
    both = jnp.where(which == 0, lax.broadcast_in_dim(source, shape, (1, 2)), gap)
    both = lax.optimization_barrier(both)
    vv = split_blocks(factor_vv)

    plane = shaped((PLANES * rows, cols))
    near = shaped((NEAR, *plane.shape))
    planes = shaped((PLANES, *plane.shape))
    half = shaped((pairs, NEAR * PLANES * 8, cols), jnp.bfloat16)
    given = along_z(jnp.broadcast_to(both[None], (PLANES, *both.shape)))
    all_source, all_gap, copies = call(first_kernel, (plane, plane, near), [VMEM], 4, 10**10)(given)
    for sweep in range(ITERS):
        if sweep:
            arrived = along_z(call(partial_kernel, planes, [VMEM], 4)(arrived))
            copies = call(next_kernel, near, [VMEM] * 3, 4)(all_source, all_gap, arrived)
        own = along_xy(copies)
        send, *halves = call(send_kernel, (near, half, half), [VMEM] * 5, 24, 10**9)(
            own, swapped(own), factor_oo, *vv
        )
        arrived = swapped(send)
        keep = call(keep_kernel, near, [VMEM] * 4, 24, 10**9)(*vv, *halves)
        arrived = along_xy(keep + arrived)
    arrived = along_z(call(total_kernel, shaped((PLANES, rows, cols)), [VMEM], 4)(arrived))
    return call(last_kernel, shaped((rows, cols)), [VMEM] * 2, 4)(both, arrived)


def solution(mesh):
    line = Mesh(mesh.devices.reshape(-1), ("d",))
    placed = (P("d", None), P("d"), P(), P("d", None, None), P("d", None, None))
    return jax.shard_map(
        local, mesh=line, in_specs=placed, out_specs=P("d", None), check_vma=False
    )
```

```python
import itertools

import jax
import jax.numpy as jnp
from jax import lax
from jax.experimental import pallas as pl
from jax.experimental.pallas import tpu as pltpu
from jax.sharding import Mesh
from jax.sharding import PartitionSpec as P

ITERS = 2
SHAPE = (8, 4, 4, 2)
PLANES, NEAR, CORES = 8, 16, 2
CHIPS = ((0, 0), (0, 1), (1, 1), (2, 1), (2, 2), (1, 2), (0, 2), (0, 3))
CHIPS += ((1, 3), (2, 3), (3, 3), (3, 2), (3, 1), (3, 0), (2, 0), (1, 0))
XY = tuple(x * SHAPE[2] + y for x, y in CHIPS)
Z = (0, 4, 1, 5, 2, 6, 3, 7)
MIB = 1024 * 1024
VMEM = pl.BlockSpec(memory_space=pltpu.VMEM)


def shaped(shape, dtype=jnp.float32):
    return jax.ShapeDtypeStruct(shape, dtype)


def call(kernel, out_shape, in_specs, mib, flops=0):
    cost = pl.CostEstimate(flops=flops, bytes_accessed=10**7, transcendentals=0)
    return pl.pallas_call(
        kernel,
        out_shape=out_shape,
        in_specs=in_specs,
        out_specs=jax.tree.map(lambda _: VMEM, out_shape),
        cost_estimate=cost if flops else None,
        compiler_params=pltpu.CompilerParams(vmem_limit_bytes=mib * MIB),
    )


def split(value):
    high = value.astype(jnp.bfloat16)
    low = (value - high.astype(jnp.float32)).astype(jnp.bfloat16)
    return high, low


def product(left, right):
    return jnp.dot(left, right, preferred_element_type=jnp.float32)


def interleaved(top, bottom):
    axis = top.ndim - 2
    head = lax.broadcasted_iota(jnp.int32, top.shape, axis) < 4
    return (
        jnp.where(head, top, pltpu.roll(bottom, 4, axis)),
        jnp.where(head, pltpu.roll(top, 4, axis), bottom),
    )


def split_kernel(value, high, low):
    def tile_at(z, at):
        return value[0, pl.ds((z * NEAR + at) * 8, 8), :]

    for n, at in enumerate(XY):
        cores = ([], [])
        for z in range(0, value.shape[1] // (NEAR * 8), 2):
            for core, tile in enumerate(interleaved(tile_at(z, at), tile_at(z + 1, at))):
                cores[core].append(tile)
        for core, tiles in enumerate(cores):
            high[0, core, n], low[0, core, n] = split(jnp.concatenate(tiles))


def split_blocks(value):
    pairs, rows, cols = value.shape
    out = shaped((pairs, CORES, NEAR, PLANES * 4, cols), jnp.bfloat16)
    block = pl.BlockSpec((1, CORES, NEAR, 16, cols), lambda p, n: (p, 0, 0, n, 0))
    return pl.pallas_call(
        split_kernel,
        grid=(pairs, PLANES // 4),
        in_specs=[pl.BlockSpec((1, 4 * NEAR * 8, cols), lambda p, n: (p, n, 0))],
        out_specs=(block, block),
        out_shape=(out, out),
        compiler_params=pltpu.CompilerParams(vmem_limit_bytes=12 * MIB),
    )(value)


def summed(arrived):
    total = arrived[0]
    for n in range(1, arrived.shape[0]):
        total = total + arrived[n]
    return total


def spread(value, copies):
    for n in range(copies.shape[0]):
        copies[n] = value


def first_kernel(given, source, gap, copies):
    for z in range(0, PLANES, 2):
        part = slice(4 * z, 4 * z + 8)
        at = Z.index(z), Z.index(z + 1)
        source[part, :] = jnp.concatenate([given[n, 0] for n in at])
        gap[part, :] = jnp.concatenate([given[n, 1] for n in at])
    spread(source[...] / gap[...], copies)


def partial_kernel(arrived, copies):
    spread(summed(arrived), copies)


def next_kernel(source, gap, arrived, copies):
    spread((source[...] - summed(arrived)) / gap[...], copies)


def total_kernel(arrived, out):
    total = summed(arrived)
    for n, z in enumerate(Z):
        out[n] = total[4 * z : 4 * z + 4, :]


def last_kernel(both, arrived, out):
    out[...] = (both[0] - summed(arrived)) / both[1]


def left_products(core, vv_high, vv_low, half_high, half_low, out):
    group = 8
    for n in range(0, NEAR, group):
        total = None
        for p in range(vv_high.shape[0]):
            high, low = (
                vv[p, core, n : n + group].reshape(group * PLANES * 4, -1)
                for vv in (vv_high, vv_low)
            )
            term = (
                product(high, half_low[p]) + product(low, half_high[p]) + product(high, half_high[p])
            )
            total = term if total is None else total + term
        out[n : n + group] = total.reshape(group, PLANES * 4, -1)


def send_kernel(own, other, oo, vv_high, vv_low, send, half_high, half_low):
    core = lax.rem(lax.axis_index("d"), CORES)
    first = core == 0
    for z in range(0, PLANES, 2):
        part = slice(4 * z, 4 * z + 8)
        ours, theirs = own[:, part, :], other[:, part, :]
        planes = interleaved(jnp.where(first, ours, theirs), jnp.where(first, theirs, ours))
        tiles = [v[XY.index(at)] for v in planes for at in range(NEAR)]
        high, low = split(jnp.concatenate(tiles))
        rows = slice(z * NEAR * 8, (z + 2) * NEAR * 8)
        for p in range(oo.shape[0]):
            oo_high, oo_low = split(oo[p])
            halfway = product(high, oo_low) + product(low, oo_high) + product(high, oo_high)
            half_high[p, rows, :], half_low[p, rows, :] = split(halfway)
    left_products(1 - core, vv_high, vv_low, half_high, half_low, send)


def keep_kernel(vv_high, vv_low, half_high, half_low, keep):
    core = lax.rem(lax.axis_index("d"), CORES)
    left_products(core, vv_high, vv_low, half_high, half_low, keep)


def device(z, x, y, c):
    _, xs, ys, cores = SHAPE
    return ((z * xs + x) * ys + y) * cores + c


def every():
    return itertools.product(*(range(n) for n in SHAPE))


def swapped(value):
    pairs = [(device(z, x, y, c), device(z, x, y, 1 - c)) for z, x, y, c in every()]
    return lax.ppermute(value, "d", pairs)


def exchanged(value, kept):
    groups = {}
    for spot in sorted(every(), key=lambda s: (Z.index(s[0]), CHIPS.index(s[1:3]), s[3])):
        groups.setdefault(tuple(spot[k] for k in kept), []).append(device(*spot))
    groups = list(groups.values())
    return lax.all_to_all(value, "d", 0, 0, axis_index_groups=groups, tiled=True)


def along_z(value):
    return exchanged(value, (1, 2, 3))


def along_xy(value):
    return exchanged(value, (0, 3))


def local(source, vir_energy, occ_energy, factor_vv, factor_oo):
    rows, cols = source.shape
    pairs = factor_oo.shape[0]

    shape = (2, rows, cols)
    gap = lax.broadcast_in_dim(vir_energy, shape, (1,)) - lax.broadcast_in_dim(occ_energy, shape, (2,))
    which = lax.broadcasted_iota(jnp.int32, shape, 0)
    both = jnp.where(which == 0, lax.broadcast_in_dim(source, shape, (1, 2)), gap)
    both = lax.optimization_barrier(both)
    vv = split_blocks(factor_vv)

    plane = shaped((PLANES * rows, cols))
    near = shaped((NEAR, *plane.shape))
    planes = shaped((PLANES, *plane.shape))
    half = shaped((pairs, NEAR * PLANES * 8, cols), jnp.bfloat16)
    given = along_z(jnp.broadcast_to(both[None], (PLANES, *both.shape)))
    all_source, all_gap, copies = call(first_kernel, (plane, plane, near), [VMEM], 4, 10**10)(given)
    for sweep in range(ITERS):
        if sweep:
            arrived = along_z(call(partial_kernel, planes, [VMEM], 4)(arrived))
            copies = call(next_kernel, near, [VMEM] * 3, 4)(all_source, all_gap, arrived)
        own = along_xy(copies)
        send, *halves = call(send_kernel, (near, half, half), [VMEM] * 5, 24, 10**9)(
            own, swapped(own), factor_oo, *vv
        )
        arrived = swapped(send)
        keep = call(keep_kernel, near, [VMEM] * 4, 24, 10**9)(*vv, *halves)
        arrived = along_xy(keep + arrived)
    arrived = along_z(call(total_kernel, shaped((PLANES, rows, cols)), [VMEM], 4)(arrived))
    return call(last_kernel, shaped((rows, cols)), [VMEM] * 2, 4)(both, arrived)


def solution(mesh):
    line = Mesh(mesh.devices.reshape(-1), ("d",))
    placed = (P("d", None), P("d"), P(), P("d", None, None), P("d", None, None))
    return jax.shard_map(
        local, mesh=line, in_specs=placed, out_specs=P("d", None), check_vma=False
    )
```
